32 devices in a mesh: groups: 2 (over y), dp: 2 (over core), tensor: 8 (over z, x).
Axes of the slice: x: 2, y: 2, z: 4, core: 2. Of those that a mesh axis runs over, the one named last changes fastest.
Arguments:
- hidden_in: bfloat16 [4, 1024, 5120], P(('groups', 'dp'), 'tensor'), parts along dimension 0, may hold values from -40 to 40
- first_values: bfloat16 [4, 1024, 1024], P(('groups', 'dp'), 'tensor'), parts along dimension 0, may hold values from -6 to 6
- qkv_weight: bfloat16 [5120, 3, 1024], P(None, None, 'tensor'), may hold values from -1 to 1
- out_weight: bfloat16 [1024, 5120], P('tensor'), may hold values from -0.1875 to 0.1875
- mix_table: float32 [8, 2], replicated, may hold values from 0.2 to 1
- mix_index: int32 [8], P('tensor'), may hold values from 0 to 7
- lengths: int32 [4], P(('groups', 'dp')), parts along dimension 0, may hold values from 256 to 1024
Outputs:
- attn_out: bfloat16 [4, 1024, 5120], P(('groups', 'dp'), 'tensor'), parts along dimension 0
The draws below stay inside these ranges and needn't reach their ends.
There are 2 independent parts, one for each index of `groups`. The reference program is written for one: setup_inputs(seed, part) draws one part's arguments, and reference() takes and returns one part's arrays. A program takes and returns all parts, laid end to end along the dimension named above; an argument that names none is the same for every part. Nothing has to cross between parts.
All inputs are finite; a program needn't handle non-finite values.
Results may differ from the reference program's by a relative error of at most 0.0077.
Values may be sent and summed in bfloat16 or wider, within the bound.
A program may use at most 128 MiB of HBM per device.

```python
import math
import jax
import jax.numpy as jnp
from jax import lax

D = 5120
HS = 128
MIXES = 8
SEQ = 1024
HEADS = 8
SEQS = 2


def draw_hidden_in(key, part):
    samples = jnp.clip(jax.random.normal(jax.random.fold_in(key, 11), (SEQS, SEQ, D), jnp.float32), -6.0, 6.0)
    return samples.astype(jnp.bfloat16)


def draw_qkv_weight(key, part):
    inner_width = HEADS * HS
    spread = 1.0 / math.sqrt(D)
    weights = jax.random.normal(jax.random.fold_in(key, 21), (D, 3, inner_width), jnp.float32) * spread
    return jnp.clip(weights, -1.0, 1.0).astype(jnp.bfloat16)


def with_ends(drawn, own_key, least, top_value):
    longest = drawn.shape.index(max(drawn.shape))
    spots = []
    for shift in (0, 1):
        where = [jax.random.randint(jax.random.fold_in(own_key, axis), (), 0, length) for axis, length in enumerate(drawn.shape)]
        where[longest] = (where[longest] + shift) % drawn.shape[longest]
        spots.append(tuple(where))
    return drawn.at[spots[0]].set(least).at[spots[1]].set(top_value)


def level_of(key, dims, cuts, smallest, high):
    gain, own = 1.0, jax.random.fold_in(key, 6)
    for position, shards_of in cuts:
        steps = jnp.exp(jax.random.uniform(jax.random.fold_in(own, position), (shards_of,), jnp.float32, smallest / len(cuts), high / len(cuts)))
        gain = gain * jnp.repeat(steps, dims[position] // shards_of).reshape([-1 if axis == position else 1 for axis in range(len(dims))])
    return gain


def scatter_about(stream_key, dims, width, limit, shards=(), kind=jnp.bfloat16):
    values = width * jax.random.normal(stream_key, dims, jnp.float32)
    if shards:
        values = values * level_of(stream_key, dims, shards, -0.22, 0.18)
    return jnp.clip(values, -limit, limit).astype(kind)


def setup_inputs(seed: int = 0, part: int = 0) -> dict:
    splits = jax.random.split(jax.random.key(seed), 8)
    own_keys = jax.random.split(jax.random.fold_in(splits[7], part), 8)
    hidden_in = draw_hidden_in(jax.random.fold_in(jax.random.fold_in(splits[7], part), 71), part)
    first_values = scatter_about(own_keys[1], (SEQS, SEQ, HEADS * HS), 1.0, 6.0, ((0, 2), (1, 8)))
    qkv_weight = draw_qkv_weight(jax.random.fold_in(splits[7], 71), part)
    out_weight = scatter_about(splits[3], (HEADS * HS, D), (8 * HS) ** -0.5, 0.1875, ((0, 8),))
    mix_table = jnp.clip(jax.random.uniform(splits[4], (MIXES, 2), jnp.float32, 0.2, 1.0), 0.2, 1.0)
    mix_index = with_ends(jax.random.randint(splits[5], (HEADS,), 0, MIXES), jax.random.fold_in(splits[5], 1), 0, MIXES - 1).astype(jnp.int32)
    lengths = jax.random.randint(own_keys[6], (SEQS,), SEQ // 4, SEQ + 1).astype(jnp.int32)
    return {"hidden_in": hidden_in, "first_values": first_values, "qkv_weight": qkv_weight, "out_weight": out_weight, "mix_table": mix_table, "mix_index": mix_index, "lengths": lengths}


NEG_FILL = -1e+30

def reference(hidden_in, first_values, qkv_weight, out_weight, mix_table, mix_index, lengths):
    merged_weight = qkv_weight.reshape(D, 3 * HEADS * HS)
    lambdas = mix_table[mix_index]
    score_scale = 1.0 / math.sqrt(HS)
    positions = jnp.arange(SEQ, dtype=jnp.int32)

    def one_sequence(packed):
        tok_rows, firsts, valid_length = packed
        projected = jnp.dot(tok_rows, merged_weight, preferred_element_type=jnp.float32).astype(jnp.bfloat16)
        split_parts = projected.reshape(SEQ, 3, HEADS, HS)
        first_float = firsts.reshape(SEQ, HEADS, HS).astype(jnp.float32)
        value_float = split_parts[:, 2].astype(jnp.float32)
        mixed_values = (lambdas[None, :, 0:1] * value_float + lambdas[None, :, 1:2] * first_float).astype(jnp.bfloat16)
        allowed = (positions[None, :] <= positions[:, None]) & (positions[None, :] < valid_length)

        def one_head(items):
            query_rows, key_rows, value_rows = items
            scores = jnp.dot(query_rows, key_rows.T, preferred_element_type=jnp.float32) * score_scale
            scores = jnp.where(allowed, scores, NEG_FILL)
            row_max = lax.optimization_barrier(jnp.max(scores, axis=1, keepdims=True))
            raised = jnp.exp(scores - row_max)
            weights = (raised / lax.optimization_barrier(jnp.sum(raised, axis=1, keepdims=True))).astype(jnp.bfloat16)
            return jnp.dot(weights, value_rows, preferred_element_type=jnp.float32).astype(jnp.bfloat16)
        per_head = lax.map(one_head, (jnp.transpose(split_parts[:, 0], (1, 0, 2)), jnp.transpose(split_parts[:, 1], (1, 0, 2)), jnp.transpose(mixed_values, (1, 0, 2))))
        attended = jnp.transpose(per_head, (1, 0, 2)).reshape(SEQ, HEADS * HS)
        return jnp.dot(attended, out_weight, preferred_element_type=jnp.float32).astype(jnp.bfloat16)
    return lax.map(one_sequence, (hidden_in, first_values, lengths))
```

```python
import math

import jax
import jax.numpy as jnp
from jax import lax
from jax.sharding import PartitionSpec as P

NEG_FILL = -1e30
PAIR = 2


def attention(queries, key_rows, mixed_values, valid_length, head_size):
    total_rows = queries.shape[0]
    positions = jnp.arange(total_rows, dtype=jnp.int32)
    score_scale = 1.0 / math.sqrt(head_size)
    block_rows = min(512, total_rows)
    outputs = []
    for first_row in range(0, total_rows, block_rows):
        stop = first_row + block_rows
        scores = (
            jnp.einsum(
                "qhd,khd->hqk",
                queries[first_row:stop],
                key_rows[:stop],
                preferred_element_type=jnp.float32,
            )
            * score_scale
        )
        keys_at, rows_at = positions[:stop], positions[first_row:stop]
        allowed = (keys_at[None, :] <= rows_at[:, None]) & (keys_at[None, :] < valid_length)
        scores = jnp.where(allowed[None], scores, NEG_FILL)
        row_max = jnp.max(scores, axis=2, keepdims=True)
        raised = jnp.exp(scores - row_max)
        weights = (raised / jnp.sum(raised, axis=2, keepdims=True)).astype(jnp.bfloat16)
        outputs.append(
            jnp.einsum(
                "hqk,khd->qhd", weights, mixed_values[:stop], preferred_element_type=jnp.float32
            ).astype(jnp.bfloat16)
        )
    return jnp.concatenate(outputs, axis=0)


def body(hidden_in, first_values, qkv_weight, out_weight, mix_table, mix_index, lengths):
    local_rows = hidden_in[0]
    own_rows, model_width = local_rows.shape
    head_width = qkv_weight.shape[2]
    heads_here = mix_index.shape[0]
    head_size = head_width // heads_here
    ranks = lax.axis_size("tensor")
    cores = lax.axis_size("dp")
    rank = lax.axis_index("tensor")
    core = lax.axis_index("dp")
    side = rank % PAIR
    line = ranks // PAIR
    swap_pair = [(r, r ^ 1) for r in range(ranks)]
    swap_core = [(c, c ^ 1) for c in range(cores)]

    own_w = qkv_weight.reshape(model_width, 3 * head_width)
    half = model_width // 2
    sent = lax.dynamic_slice_in_dim(own_w, core * half, half, 0)
    got = lax.ppermute(sent, "tensor", swap_pair)
    got_other = lax.ppermute(got, "dp", swap_core)
    pair_w = jnp.where(
        core == 0,
        jnp.concatenate([got, got_other], axis=0),
        jnp.concatenate([got_other, got], axis=0),
    )

    lines = [[s + PAIR * i for i in range(line)] for s in range(PAIR)]
    rows = lax.all_gather(local_rows, "tensor", axis=0, tiled=True, axis_index_groups=lines)
    for_pair = jnp.dot(rows, pair_w, preferred_element_type=jnp.float32).astype(jnp.bfloat16)
    from_pair = lax.ppermute(for_pair, "tensor", swap_pair)
    ours = jnp.dot(rows, own_w, preferred_element_type=jnp.float32).astype(jnp.bfloat16)
    ours = ours.reshape(line, own_rows, 3 * head_width)
    from_pair = from_pair.reshape(line, own_rows, 3 * head_width)
    projected = jnp.where(
        side == 0,
        jnp.stack([ours, from_pair], axis=1),
        jnp.stack([from_pair, ours], axis=1),
    )
    total_rows = ranks * own_rows
    split_parts = projected.reshape(total_rows, 3, heads_here, head_size)

    relaid = lax.all_to_all(first_values[0], "tensor", split_axis=1, concat_axis=0, tiled=True)
    firsts = relaid.reshape(total_rows, heads_here, head_size)
    levels = mix_table.shape[0]
    one_hot = (mix_index[:, None] == jnp.arange(levels, dtype=jnp.int32)[None, :]).astype(
        jnp.float32
    )
    weights_mix = jnp.dot(one_hot, mix_table, precision=lax.Precision.HIGHEST)
    mixed_values = (
        weights_mix[None, :, 0:1] * split_parts[:, 2].astype(jnp.float32)
        + weights_mix[None, :, 1:2] * firsts.astype(jnp.float32)
    ).astype(jnp.bfloat16)
    attended = attention(
        split_parts[:, 0], split_parts[:, 1], mixed_values, lengths[0], head_size
    ).reshape(total_rows, head_width)

    gathered_bytes = ranks * out_weight.size * 2
    summed_bytes = total_rows * model_width * 4
    if gathered_bytes > summed_bytes:
        kept_rows = lax.psum_scatter(
            jnp.dot(attended, out_weight, preferred_element_type=jnp.float32),
            "tensor",
            scatter_dimension=0,
            tiled=True,
        )
        return kept_rows.astype(jnp.bfloat16)[None]

    part = head_width // 2
    own_part = lax.dynamic_slice_in_dim(out_weight, core * part, part, 0)
    mine = lax.all_gather(own_part, "tensor", axis=0, tiled=True)
    other = lax.ppermute(mine, "dp", swap_core)
    kept = lax.all_to_all(attended, "tensor", split_axis=0, concat_axis=1, tiled=True)
    kept = kept.reshape(own_rows, ranks, 2, part)
    low = kept[:, :, 0].reshape(own_rows, ranks * part)
    high = kept[:, :, 1].reshape(own_rows, ranks * part)
    out = jnp.dot(
        jnp.where(core == 0, low, high), mine, preferred_element_type=jnp.float32
    ) + jnp.dot(jnp.where(core == 0, high, low), other, preferred_element_type=jnp.float32)
    return out.astype(jnp.bfloat16)[None]


def solution(mesh):
    placed = (
        P(("groups", "dp"), "tensor", None),
        P(("groups", "dp"), "tensor", None),
        P(None, None, "tensor"),
        P("tensor", None),
        P(),
        P("tensor"),
        P(("groups", "dp")),
    )
    return jax.shard_map(
        body,
        mesh=mesh,
        in_specs=placed,
        out_specs=P(("groups", "dp"), "tensor", None),
        check_vma=False,
    )
```

```python
import functools
import math

import jax
import jax.numpy as jnp
from jax import lax
from jax.experimental import pallas as pl
from jax.experimental.pallas import tpu as pltpu
from jax.sharding import PartitionSpec as P

NEG_FILL = -1e30
PAIR = 2


def attention(queries, key_rows, mixed_values, valid_length, head_size):
    total_rows = queries.shape[0]
    positions = jnp.arange(total_rows, dtype=jnp.int32)
    score_scale = 1.0 / math.sqrt(head_size)
    block_rows = min(512, total_rows)
    outputs = []
    for first_row in range(0, total_rows, block_rows):
        stop = first_row + block_rows
        scores = (
            jnp.einsum(
                "qhd,khd->hqk",
                queries[first_row:stop],
                key_rows[:stop],
                preferred_element_type=jnp.float32,
            )
            * score_scale
        )
        keys_at, rows_at = positions[:stop], positions[first_row:stop]
        allowed = (keys_at[None, :] <= rows_at[:, None]) & (keys_at[None, :] < valid_length)
        scores = jnp.where(allowed[None], scores, NEG_FILL)
        row_max = jnp.max(scores, axis=2, keepdims=True)
        raised = jnp.exp(scores - row_max)
        weights = (raised / jnp.sum(raised, axis=2, keepdims=True)).astype(jnp.bfloat16)
        outputs.append(
            jnp.einsum(
                "hqk,khd->qhd", weights, mixed_values[:stop], preferred_element_type=jnp.float32
            ).astype(jnp.bfloat16)
        )
    return jnp.concatenate(outputs, axis=0)


def body(hidden_in, first_values, qkv_weight, out_weight, mix_table, mix_index, lengths):
    local_rows = hidden_in[0]
    own_rows, model_width = local_rows.shape
    head_width = qkv_weight.shape[2]
    heads_here = mix_index.shape[0]
    head_size = head_width // heads_here
    ranks = lax.axis_size("tensor")
    cores = lax.axis_size("dp")
    rank = lax.axis_index("tensor")
    core = lax.axis_index("dp")
    side = rank % PAIR
    line = ranks // PAIR
    swap_pair = [(r, r ^ 1) for r in range(ranks)]
    swap_core = [(c, c ^ 1) for c in range(cores)]

    own_w = qkv_weight.reshape(model_width, 3 * head_width)
    half = model_width // 2
    sent = lax.dynamic_slice_in_dim(own_w, core * half, half, 0)
    got = lax.ppermute(sent, "tensor", swap_pair)
    got_other = lax.ppermute(got, "dp", swap_core)
    pair_w = jnp.where(
        core == 0,
        jnp.concatenate([got, got_other], axis=0),
        jnp.concatenate([got_other, got], axis=0),
    )

    lines = [[s + PAIR * i for i in range(line)] for s in range(PAIR)]
    rows = lax.all_gather(local_rows, "tensor", axis=0, tiled=True, axis_index_groups=lines)
    for_pair = jnp.dot(rows, pair_w, preferred_element_type=jnp.float32).astype(jnp.bfloat16)
    from_pair = lax.ppermute(for_pair, "tensor", swap_pair)
    ours = jnp.dot(rows, own_w, preferred_element_type=jnp.float32).astype(jnp.bfloat16)
    ours = ours.reshape(line, own_rows, 3 * head_width)
    from_pair = from_pair.reshape(line, own_rows, 3 * head_width)
    projected = jnp.where(
        side == 0,
        jnp.stack([ours, from_pair], axis=1),
        jnp.stack([from_pair, ours], axis=1),
    )
    total_rows = ranks * own_rows
    split_parts = projected.reshape(total_rows, 3, heads_here, head_size)

    relaid = lax.all_to_all(first_values[0], "tensor", split_axis=1, concat_axis=0, tiled=True)
    firsts = relaid.reshape(total_rows, heads_here, head_size)
    levels = mix_table.shape[0]
    one_hot = (mix_index[:, None] == jnp.arange(levels, dtype=jnp.int32)[None, :]).astype(
        jnp.float32
    )
    weights_mix = jnp.dot(one_hot, mix_table, precision=lax.Precision.HIGHEST)
    mixed_values = (
        weights_mix[None, :, 0:1] * split_parts[:, 2].astype(jnp.float32)
        + weights_mix[None, :, 1:2] * firsts.astype(jnp.float32)
    ).astype(jnp.bfloat16)
    attended = attention(
        split_parts[:, 0], split_parts[:, 1], mixed_values, lengths[0], head_size
    ).reshape(total_rows, head_width)

    gathered_bytes = ranks * out_weight.size * 2
    summed_bytes = total_rows * model_width * 4
    if gathered_bytes > summed_bytes:
        kept_rows = lax.psum_scatter(
            jnp.dot(attended, out_weight, preferred_element_type=jnp.float32),
            "tensor",
            scatter_dimension=0,
            tiled=True,
        )
        return kept_rows.astype(jnp.bfloat16)[None]

    part = head_width // 2
    own_part = lax.dynamic_slice_in_dim(out_weight, core * part, part, 0)
    mine = lax.all_gather(own_part, "tensor", axis=0, tiled=True)
    other = lax.ppermute(mine, "dp", swap_core)
    kept = lax.all_to_all(attended, "tensor", split_axis=0, concat_axis=1, tiled=True)
    kept = kept.reshape(own_rows, ranks, 2, part)
    low = kept[:, :, 0].reshape(own_rows, ranks * part)
    high = kept[:, :, 1].reshape(own_rows, ranks * part)
    out = jnp.dot(
        jnp.where(core == 0, low, high), mine, preferred_element_type=jnp.float32
    ) + jnp.dot(jnp.where(core == 0, high, low), other, preferred_element_type=jnp.float32)
    return out.astype(jnp.bfloat16)[None]


PIECES = 2
MESH = pl.DeviceIdType.MESH


def gather_project(
    line, rows_ref, w_ref, ow_ref, qkv_ref, wf_ref,
    hid, own_w, pair_w, own_o, staged,
    load_sem, hs_sem, hr_sem, ws_sem, wr_sem, os_sem, or_sem, xs_sem, xr_sem,
    ys_sem, yr_sem, ds_sem, dr_sem, es_sem, er_sem, ps_sem, pr_sem,
):
    group, core, rank = lax.axis_index("groups"), lax.axis_index("dp"), lax.axis_index("tensor")
    spot, side = rank // PAIR, rank % PAIR
    steps = line - 1
    own_rows, width = rows_ref.shape
    half = width // 2
    quarter = ow_ref.shape[0] // 4
    mine = group * 2 + core
    across = (1 - group) * 2 + core
    left, right = (group, core, rank - PAIR), (group, core, rank + PAIR)
    partner = (group, core, spot * PAIR + 1 - side)
    opposite = (1 - group, core, rank)
    sibling = (group, 1 - core, rank)
    has_left, has_right = spot > 0, spot < steps

    barrier = pltpu.get_barrier_semaphore()
    for there in (partner, opposite, sibling):
        pl.semaphore_signal(barrier, inc=1, device_id=there, device_id_type=MESH)

    @pl.when(has_left)
    def _():
        pl.semaphore_signal(barrier, inc=1, device_id=left, device_id_type=MESH)

    @pl.when(has_right)
    def _():
        pl.semaphore_signal(barrier, inc=1, device_id=right, device_id_type=MESH)

    loads = [
        pltpu.make_async_copy(rows_ref, hid.at[spot], load_sem.at[0]),
        pltpu.make_async_copy(ow_ref, own_o, load_sem.at[1]),
        pltpu.make_async_copy(w_ref, own_w, load_sem.at[2]),
    ]
    for load in loads:
        load.start()
    pl.semaphore_wait(barrier, 3 + jnp.where(has_left, 1, 0) + jnp.where(has_right, 1, 0))

    def send(src, dst, s_sem, r_sem, there):
        return pltpu.make_async_remote_copy(
            src_ref=src, dst_ref=dst, send_sem=s_sem, recv_sem=r_sem, device_id=there, device_id_type=MESH
        )

    def wf(column, q):
        return wf_ref.at[column, pl.ds(q * quarter, quarter), :]

    def chunk(way, k):
        return spot - 1 - k if way == 0 else spot + 1 + k

    def arrives(way, k):
        return k < spot if way == 0 else spot + 1 + k < line

    def leaves(way, k):
        if way == 0:
            return jnp.logical_and(k <= spot, has_right)
        return jnp.logical_and(spot + k < line, has_left)

    def carried(way, k):
        return spot - k if way == 0 else spot + k

    def ahead(way):
        return right if way == 0 else left

    piece = own_rows // PIECES

    def hid_copy(way, k, p, at):
        cut = pl.ds(p * piece, piece)
        source = rows_ref.at[cut, :] if k == 0 else hid.at[at, cut, :]
        return send(source, hid.at[at, cut, :], hs_sem.at[way, k, p], hr_sem.at[way, k, p], ahead(way))

    def out_copy(way, k, at):
        column = at * PAIR + side
        source = ow_ref.at[pl.ds(mine * quarter, quarter), :] if k == 0 else wf(column, mine)
        return send(source, wf(column, mine), os_sem.at[way, k], or_sem.at[way, k], ahead(way))

    def pair_copy(slot, column, source):
        return send(source, wf(column, mine), xs_sem.at[slot], xr_sem.at[slot], partner)

    def y_copy(slot, column):
        return send(wf(column, mine), wf(column, mine), ys_sem.at[slot], yr_sem.at[slot], opposite)

    def y_arrival(slot, column):
        return send(wf(column, across), wf(column, across), ys_sem.at[slot], yr_sem.at[slot], opposite)

    def d_copy(slot, column, q):
        return send(wf(column, q), wf(column, q), ds_sem.at[slot], dr_sem.at[slot], sibling)

    def e_copy(slot, column, q):
        return send(wf(column, q), wf(column, q), es_sem.at[slot], er_sem.at[slot], sibling)

    def spread(slot, column):
        y_copy(slot, column).start()
        d_copy(slot, column, mine).start()

    last = 2 * steps
    all_slots = [(way * steps + k, way, k) for k in range(steps) for way in (0, 1)]
    partner_column = spot * PAIR + 1 - side

    for way in (0, 1):

        @pl.when(leaves(way, 0))
        def _():
            out_copy(way, 0, spot).start()
            for p in range(PIECES):
                hid_copy(way, 0, p, spot).start()

    own_quarter = ow_ref.at[pl.ds(mine * quarter, quarter), :]
    pair_copy(last, rank, own_quarter).start()
    cut_w = pl.ds(core * half, half)
    other_w = pl.ds((1 - core) * half, half)
    w_out = send(w_ref.at[:, cut_w, :], pair_w.at[:, cut_w, :], ws_sem.at[0], wr_sem.at[0], partner)
    w_out.start()
    for load in loads:
        load.wait()
    keep = pltpu.make_async_copy(own_o, wf_ref.at[rank], load_sem.at[3])
    keep.start()

    def project(at, weights, store):
        def one(j, carry):
            total = jnp.dot(hid[at], weights[j], preferred_element_type=jnp.float32)
            store(j, total.astype(jnp.bfloat16))
            return carry

        lax.fori_loop(0, 3, one, 0)

    def project_own(at):
        def store(j, value):
            qkv_ref[j, at, side] = value

        project(at, own_w, store)

    def swap_copy(slot, at):
        return send(
            staged.at[slot], qkv_ref.at[:, at, side], ps_sem.at[slot], pr_sem.at[slot], partner
        )

    def swap_arrival(slot, at):
        return send(
            staged.at[slot], qkv_ref.at[:, at, 1 - side], ps_sem.at[slot], pr_sem.at[slot], partner
        )

    def project_pair(slot, at):
        def store(j, value):
            staged[slot, j] = value

        project(at, pair_w, store)

    project_own(spot)

    for k in range(steps):
        for way in (0, 1):

            @pl.when(arrives(way, k))
            def _():
                at = chunk(way, k)
                out_copy(way, k, at).wait_recv()
                if k + 1 < steps:

                    @pl.when(leaves(way, k + 1))
                    def _():
                        out_copy(way, k + 1, at).start()

                slot = way * steps + k
                column = at * PAIR + side
                pair_copy(slot, column, wf(column, mine)).start()
                spread(slot, column)

        for p in range(PIECES):
            for way in (0, 1):

                @pl.when(arrives(way, k))
                def _():
                    at = chunk(way, k)
                    hid_copy(way, k, p, at).wait_recv()
                    if k + 1 < steps:

                        @pl.when(leaves(way, k + 1))
                        def _():
                            hid_copy(way, k + 1, p, at).start()

        if k == 0:
            pair_copy(last, partner_column, wf(partner_column, mine)).wait_recv()
            spread(2 * last, partner_column)
            send(
                w_ref.at[:, cut_w, :], pair_w.at[:, cut_w, :], ws_sem.at[0], wr_sem.at[0], partner
            ).wait_recv()
            w_side = send(
                pair_w.at[:, cut_w, :], pair_w.at[:, cut_w, :], ws_sem.at[1], wr_sem.at[1], sibling
            )
            w_side.start()
            send(
                pair_w.at[:, other_w, :], pair_w.at[:, other_w, :], ws_sem.at[1], wr_sem.at[1], sibling
            ).wait_recv()
            project_pair(last, spot)
        for way in (0, 1):

            @pl.when(arrives(way, k))
            def _():
                at = chunk(way, k)
                slot = way * steps + k
                project_pair(slot, at)
                project_own(at)
                swap_copy(slot, at).start()
                column = at * PAIR + 1 - side
                pair_copy(slot, column, wf(column, mine)).wait_recv()
                spread(last + slot, column)

        if k == 0:
            swap_copy(last, spot).start()

    columns = [(2 * last, partner_column, None)]
    for slot, way, k in all_slots:
        columns.append((slot, chunk(way, k) * PAIR + side, (way, k)))
        columns.append((last + slot, chunk(way, k) * PAIR + 1 - side, (way, k)))

    def each(action):
        for slot, column, when in columns:
            if when is None:
                action(slot, column)
            else:

                @pl.when(arrives(*when))
                def _():
                    action(slot, column)

    def pass_on(slot, column):
        y_arrival(slot, column).wait_recv()
        e_copy(slot, column, across).start()

    def finish(slot, column):
        sib_mine = group * 2 + 1 - core
        sib_across = (1 - group) * 2 + 1 - core
        d_copy(slot, column, sib_mine).wait_recv()
        e_copy(slot, column, sib_across).wait_recv()
        y_copy(slot, column).wait_send()
        d_copy(slot, column, mine).wait_send()
        e_copy(slot, column, across).wait_send()

    each(pass_on)
    each(finish)
    for slot, way, k in all_slots:

        @pl.when(arrives(way, k))
        def _():
            at = chunk(way, k)
            swap_arrival(slot, at).wait_recv()
            swap_copy(slot, at).wait_send()
            column = at * PAIR + side
            pair_copy(slot, column, wf(column, mine)).wait_send()

        @pl.when(leaves(way, k))
        def _():
            at = carried(way, k)
            out_copy(way, k, at).wait_send()
            for p in range(PIECES):
                hid_copy(way, k, p, at).wait_send()

    swap_arrival(last, spot).wait_recv()
    swap_copy(last, spot).wait_send()
    pair_copy(last, rank, own_quarter).wait_send()
    w_out.wait_send()
    w_side.wait_send()
    keep.wait()


def gathered(local_rows, w3, out_weight, ranks):
    line = ranks // PAIR
    steps = line - 1
    own_rows, width = local_rows.shape
    head_width = w3.shape[2]
    kind = local_rows.dtype
    dma = pltpu.SemaphoreType.DMA
    slots, wide = 2 * steps + 1, 4 * steps + 1
    anywhere = pl.BlockSpec(memory_space=pltpu.HBM)
    return pl.pallas_call(
        functools.partial(gather_project, line),
        out_shape=(
            jax.ShapeDtypeStruct((3, line, PAIR, own_rows, head_width), kind),
            jax.ShapeDtypeStruct((ranks,) + out_weight.shape, kind),
        ),
        in_specs=[anywhere] * 3,
        out_specs=(pl.BlockSpec(memory_space=pltpu.VMEM), anywhere),
        scratch_shapes=[
            pltpu.VMEM((line, own_rows, width), kind),
            pltpu.VMEM(w3.shape, kind),
            pltpu.VMEM(w3.shape, kind),
            pltpu.VMEM(out_weight.shape, kind),
            pltpu.VMEM((slots, 3, own_rows, head_width), kind),
            dma((4,)),
            dma((2, steps, PIECES)), dma((2, steps, PIECES)),
            dma((2,)), dma((2,)),
            dma((2, steps)), dma((2, steps)),
            dma((slots,)), dma((slots,)),
            dma((wide,)), dma((wide,)),
            dma((wide,)), dma((wide,)),
            dma((wide,)), dma((wide,)),
            dma((slots,)), dma((slots,)),
        ],
        compiler_params=pltpu.CompilerParams(
            collective_id=0, has_side_effects=True, vmem_limit_bytes=48 * 1024 * 1024
        ),
    )(local_rows, w3, out_weight)


def mix(values, firsts, mix_table, mix_index):
    levels = mix_table.shape[0]
    one_hot = (mix_index[:, None] == jnp.arange(levels, dtype=jnp.int32)[None, :]).astype(
        jnp.float32
    )
    weights_mix = jnp.dot(one_hot, mix_table, precision=lax.Precision.HIGHEST)
    return (
        weights_mix[None, :, 0:1] * values.astype(jnp.float32)
        + weights_mix[None, :, 1:2] * firsts.astype(jnp.float32)
    ).astype(jnp.bfloat16)


def body_gathered(hidden_in, first_values, qkv_weight, out_weight, mix_table, mix_index, lengths):
    local_rows = hidden_in[0]
    own_rows = local_rows.shape[0]
    ranks = lax.axis_size("tensor")
    total_rows = ranks * own_rows
    heads_here = mix_index.shape[0]
    head_width = qkv_weight.shape[2]
    head_size = head_width // heads_here
    relaid = lax.all_to_all(first_values[0], "tensor", split_axis=1, concat_axis=0, tiled=True)
    firsts = relaid.reshape(total_rows, heads_here, head_size)
    qkv, full_out = gathered(local_rows, qkv_weight.transpose(1, 0, 2), out_weight, ranks)
    qkv = qkv.reshape(3, total_rows, heads_here, head_size)
    mixed_values = mix(qkv[2], firsts, mix_table, mix_index)
    attended = attention(qkv[0], qkv[1], mixed_values, lengths[0], head_size)
    attended = attended.reshape(total_rows, head_width)
    kept = lax.all_to_all(attended, "tensor", split_axis=0, concat_axis=1, tiled=True)
    weights = full_out.reshape(ranks * head_width, full_out.shape[2])
    return jnp.dot(kept, weights, preferred_element_type=jnp.float32).astype(jnp.bfloat16)[None]


def chosen(hidden_in, first_values, qkv_weight, out_weight, mix_table, mix_index, lengths):
    args = (hidden_in, first_values, qkv_weight, out_weight, mix_table, mix_index, lengths)
    ranks = lax.axis_size("tensor")
    total_rows = ranks * hidden_in.shape[1]
    fits = ranks * out_weight.size * 2 <= total_rows * hidden_in.shape[2] * 4
    two = lax.axis_size("groups") == 2 and lax.axis_size("dp") == 2
    if fits and two:
        return body_gathered(*args)
    return body(*args)


def solution(mesh):
    placed = (
        P(("groups", "dp"), "tensor", None),
        P(("groups", "dp"), "tensor", None),
        P(None, None, "tensor"),
        P("tensor", None),
        P(),
        P("tensor"),
        P(("groups", "dp")),
    )
    return jax.shard_map(
        chosen,
        mesh=mesh,
        in_specs=placed,
        out_specs=P(("groups", "dp"), "tensor", None),
        check_vma=False,
    )
```

```python
import functools
import math

import jax
import jax.numpy as jnp
from jax import lax
from jax.experimental import pallas as pl
from jax.experimental.pallas import tpu as pltpu
from jax.sharding import PartitionSpec as P

NEG_FILL = -1e30
PAIR = 2


def attention(queries, key_rows, mixed_values, valid_length, head_size):
    total_rows = queries.shape[0]
    positions = jnp.arange(total_rows, dtype=jnp.int32)
    score_scale = 1.0 / math.sqrt(head_size)
    block_rows = min(512, total_rows)
    outputs = []
    for first_row in range(0, total_rows, block_rows):
        stop = first_row + block_rows
        scores = (
            jnp.einsum(
                "qhd,khd->hqk",
                queries[first_row:stop],
                key_rows[:stop],
                preferred_element_type=jnp.float32,
            )
            * score_scale
        )
        keys_at, rows_at = positions[:stop], positions[first_row:stop]
        allowed = (keys_at[None, :] <= rows_at[:, None]) & (keys_at[None, :] < valid_length)
        scores = jnp.where(allowed[None], scores, NEG_FILL)
        row_max = jnp.max(scores, axis=2, keepdims=True)
        raised = jnp.exp(scores - row_max)
        weights = (raised / jnp.sum(raised, axis=2, keepdims=True)).astype(jnp.bfloat16)
        outputs.append(
            jnp.einsum(
                "hqk,khd->qhd", weights, mixed_values[:stop], preferred_element_type=jnp.float32
            ).astype(jnp.bfloat16)
        )
    return jnp.concatenate(outputs, axis=0)


def body(hidden_in, first_values, qkv_weight, out_weight, mix_table, mix_index, lengths):
    local_rows = hidden_in[0]
    own_rows, model_width = local_rows.shape
    head_width = qkv_weight.shape[2]
    heads_here = mix_index.shape[0]
    head_size = head_width // heads_here
    ranks = lax.axis_size("tensor")
    cores = lax.axis_size("dp")
    rank = lax.axis_index("tensor")
    core = lax.axis_index("dp")
    side = rank % PAIR
    line = ranks // PAIR
    swap_pair = [(r, r ^ 1) for r in range(ranks)]
    swap_core = [(c, c ^ 1) for c in range(cores)]

    own_w = qkv_weight.reshape(model_width, 3 * head_width)
    half = model_width // 2
    sent = lax.dynamic_slice_in_dim(own_w, core * half, half, 0)
    got = lax.ppermute(sent, "tensor", swap_pair)
    got_other = lax.ppermute(got, "dp", swap_core)
    pair_w = jnp.where(
        core == 0,
        jnp.concatenate([got, got_other], axis=0),
        jnp.concatenate([got_other, got], axis=0),
    )

    lines = [[s + PAIR * i for i in range(line)] for s in range(PAIR)]
    rows = lax.all_gather(local_rows, "tensor", axis=0, tiled=True, axis_index_groups=lines)
    for_pair = jnp.dot(rows, pair_w, preferred_element_type=jnp.float32).astype(jnp.bfloat16)
    from_pair = lax.ppermute(for_pair, "tensor", swap_pair)
    ours = jnp.dot(rows, own_w, preferred_element_type=jnp.float32).astype(jnp.bfloat16)
    ours = ours.reshape(line, own_rows, 3 * head_width)
    from_pair = from_pair.reshape(line, own_rows, 3 * head_width)
    projected = jnp.where(
        side == 0,
        jnp.stack([ours, from_pair], axis=1),
        jnp.stack([from_pair, ours], axis=1),
    )
    total_rows = ranks * own_rows
    split_parts = projected.reshape(total_rows, 3, heads_here, head_size)

    relaid = lax.all_to_all(first_values[0], "tensor", split_axis=1, concat_axis=0, tiled=True)
    firsts = relaid.reshape(total_rows, heads_here, head_size)
    levels = mix_table.shape[0]
    one_hot = (mix_index[:, None] == jnp.arange(levels, dtype=jnp.int32)[None, :]).astype(
        jnp.float32
    )
    weights_mix = jnp.dot(one_hot, mix_table, precision=lax.Precision.HIGHEST)
    mixed_values = (
        weights_mix[None, :, 0:1] * split_parts[:, 2].astype(jnp.float32)
        + weights_mix[None, :, 1:2] * firsts.astype(jnp.float32)
    ).astype(jnp.bfloat16)
    attended = attention(
        split_parts[:, 0], split_parts[:, 1], mixed_values, lengths[0], head_size
    ).reshape(total_rows, head_width)

    gathered_bytes = ranks * out_weight.size * 2
    summed_bytes = total_rows * model_width * 4
    if gathered_bytes > summed_bytes:
        kept_rows = lax.psum_scatter(
            jnp.dot(attended, out_weight, preferred_element_type=jnp.float32),
            "tensor",
            scatter_dimension=0,
            tiled=True,
        )
        return kept_rows.astype(jnp.bfloat16)[None]

    part = head_width // 2
    own_part = lax.dynamic_slice_in_dim(out_weight, core * part, part, 0)
    mine = lax.all_gather(own_part, "tensor", axis=0, tiled=True)
    other = lax.ppermute(mine, "dp", swap_core)
    kept = lax.all_to_all(attended, "tensor", split_axis=0, concat_axis=1, tiled=True)
    kept = kept.reshape(own_rows, ranks, 2, part)
    low = kept[:, :, 0].reshape(own_rows, ranks * part)
    high = kept[:, :, 1].reshape(own_rows, ranks * part)
    out = jnp.dot(
        jnp.where(core == 0, low, high), mine, preferred_element_type=jnp.float32
    ) + jnp.dot(jnp.where(core == 0, high, low), other, preferred_element_type=jnp.float32)
    return out.astype(jnp.bfloat16)[None]


PIECES = 2
MESH = pl.DeviceIdType.MESH


def gather_project(
    line, rows_ref, w_ref, ow_ref, fv_ref, qkv_ref, wf_ref, fo_ref,
    hid, both_w, own_o, staged,
    load_sem, hs_sem, hr_sem, ws_sem, wr_sem, os_sem, or_sem, xs_sem, xr_sem,
    ys_sem, yr_sem, ds_sem, dr_sem, es_sem, er_sem, ps_sem, pr_sem, fs_sem, fr_sem,
):
    group, core, rank = lax.axis_index("groups"), lax.axis_index("dp"), lax.axis_index("tensor")
    spot, side = rank // PAIR, rank % PAIR
    steps = line - 1
    own_rows, width = rows_ref.shape
    half = width // 2
    quarter = ow_ref.shape[0] // 4
    mine = group * 2 + core
    across = (1 - group) * 2 + core
    left, right = (group, core, rank - PAIR), (group, core, rank + PAIR)
    partner = (group, core, spot * PAIR + 1 - side)
    opposite = (1 - group, core, rank)
    sibling = (group, 1 - core, rank)
    has_left, has_right = spot > 0, spot < steps

    barrier = pltpu.get_barrier_semaphore()
    ranks = line * PAIR
    head = w_ref.shape[2]
    peers = [(group, core, (rank + o) % ranks) for o in range(1, ranks)]
    for there in peers + [opposite, sibling]:
        pl.semaphore_signal(barrier, inc=1, device_id=there, device_id_type=MESH)

    loads = [
        pltpu.make_async_copy(rows_ref, hid.at[spot], load_sem.at[0]),
        pltpu.make_async_copy(ow_ref, own_o, load_sem.at[1]),
        pltpu.make_async_copy(w_ref, both_w.at[:, :, pl.ds(0, head)], load_sem.at[2]),
        pltpu.make_async_copy(
            fv_ref.at[:, pl.ds(pl.multiple_of(rank * head, head), head)], fo_ref.at[rank], load_sem.at[4]
        ),
    ]
    for load in loads:
        load.start()
    pl.semaphore_wait(barrier, ranks + 1)

    def send(src, dst, s_sem, r_sem, there):
        return pltpu.make_async_remote_copy(
            src_ref=src, dst_ref=dst, send_sem=s_sem, recv_sem=r_sem, device_id=there, device_id_type=MESH
        )

    def wf(column, q):
        return wf_ref.at[column, pl.ds(q * quarter, quarter), :]

    def chunk(way, k):
        return spot - 1 - k if way == 0 else spot + 1 + k

    def arrives(way, k):
        return k < spot if way == 0 else spot + 1 + k < line

    def leaves(way, k):
        if way == 0:
            return jnp.logical_and(k <= spot, has_right)
        return jnp.logical_and(spot + k < line, has_left)

    def carried(way, k):
        return spot - k if way == 0 else spot + k

    def ahead(way):
        return right if way == 0 else left

    piece = own_rows // PIECES

    def hid_copy(way, k, p, at):
        cut = pl.ds(p * piece, piece)
        source = rows_ref.at[cut, :] if k == 0 else hid.at[at, cut, :]
        return send(source, hid.at[at, cut, :], hs_sem.at[way, k, p], hr_sem.at[way, k, p], ahead(way))

    def out_copy(way, k, at):
        column = at * PAIR + side
        source = ow_ref.at[pl.ds(mine * quarter, quarter), :] if k == 0 else wf(column, mine)
        return send(source, wf(column, mine), os_sem.at[way, k], or_sem.at[way, k], ahead(way))

    def pair_copy(slot, column, source):
        return send(source, wf(column, mine), xs_sem.at[slot], xr_sem.at[slot], partner)

    def y_copy(slot, column):
        return send(wf(column, mine), wf(column, mine), ys_sem.at[slot], yr_sem.at[slot], opposite)

    def y_arrival(slot, column):
        return send(wf(column, across), wf(column, across), ys_sem.at[slot], yr_sem.at[slot], opposite)

    def d_copy(slot, column, q):
        return send(wf(column, q), wf(column, q), ds_sem.at[slot], dr_sem.at[slot], sibling)

    def e_copy(slot, column, q):
        return send(wf(column, q), wf(column, q), es_sem.at[slot], er_sem.at[slot], sibling)

    def spread(slot, column):
        y_copy(slot, column).start()
        d_copy(slot, column, mine).start()

    last = 2 * steps
    all_slots = [(way * steps + k, way, k) for k in range(steps) for way in (0, 1)]
    partner_column = spot * PAIR + 1 - side

    for way in (0, 1):

        @pl.when(leaves(way, 0))
        def _():
            out_copy(way, 0, spot).start()
            for p in range(PIECES):
                hid_copy(way, 0, p, spot).start()

    own_quarter = ow_ref.at[pl.ds(mine * quarter, quarter), :]
    pair_copy(last, rank, own_quarter).start()
    cut_w = pl.ds(core * half, half)
    other_w = pl.ds((1 - core) * half, half)
    lanes = pl.ds(head, head)
    w_out = send(w_ref.at[:, cut_w, :], both_w.at[:, cut_w, lanes], ws_sem.at[0], wr_sem.at[0], partner)
    first_copies = [
        send(
            fv_ref.at[:, pl.ds(pl.multiple_of(there[2] * head, head), head)],
            fo_ref.at[rank], fs_sem.at[o], fr_sem.at[o], there,
        )
        for o, there in enumerate(peers)
    ]
    w_out.start()
    for copy in first_copies:
        copy.start()
    for load in loads:
        load.wait()
    keep = pltpu.make_async_copy(own_o, wf_ref.at[rank], load_sem.at[3])
    keep.start()

    def project(slot, at):
        def one(j, carry):
            total = jnp.dot(hid[at], both_w[j], preferred_element_type=jnp.float32)
            staged[slot, j] = total[:, head:].astype(jnp.bfloat16)
            qkv_ref[j, at, side] = total[:, :head].astype(jnp.bfloat16)
            return carry

        lax.fori_loop(0, 3, one, 0)

    def swap_copy(slot, at):
        return send(
            staged.at[slot], qkv_ref.at[:, at, side], ps_sem.at[slot], pr_sem.at[slot], partner
        )

    def swap_arrival(slot, at):
        return send(
            staged.at[slot], qkv_ref.at[:, at, 1 - side], ps_sem.at[slot], pr_sem.at[slot], partner
        )

    for k in range(steps):
        for way in (0, 1):

            @pl.when(arrives(way, k))
            def _():
                at = chunk(way, k)
                out_copy(way, k, at).wait_recv()
                if k + 1 < steps:

                    @pl.when(leaves(way, k + 1))
                    def _():
                        out_copy(way, k + 1, at).start()

                slot = way * steps + k
                column = at * PAIR + side
                pair_copy(slot, column, wf(column, mine)).start()
                spread(slot, column)

        for p in range(PIECES):
            for way in (0, 1):

                @pl.when(arrives(way, k))
                def _():
                    at = chunk(way, k)
                    hid_copy(way, k, p, at).wait_recv()
                    if k + 1 < steps:

                        @pl.when(leaves(way, k + 1))
                        def _():
                            hid_copy(way, k + 1, p, at).start()

        if k == 0:
            pair_copy(last, partner_column, wf(partner_column, mine)).wait_recv()
            spread(2 * last, partner_column)
            send(
                w_ref.at[:, cut_w, :], both_w.at[:, cut_w, lanes], ws_sem.at[0], wr_sem.at[0], partner
            ).wait_recv()
            w_side = send(
                both_w.at[:, cut_w, lanes], both_w.at[:, cut_w, lanes], ws_sem.at[1], wr_sem.at[1], sibling
            )
            w_side.start()
            send(
                both_w.at[:, other_w, lanes], both_w.at[:, other_w, lanes], ws_sem.at[1], wr_sem.at[1], sibling
            ).wait_recv()
            project(last, spot)
        for way in (0, 1):

            @pl.when(arrives(way, k))
            def _():
                at = chunk(way, k)
                slot = way * steps + k
                project(slot, at)
                column = at * PAIR + 1 - side
                pair_copy(slot, column, wf(column, mine)).wait_recv()
                spread(last + slot, column)
                swap_copy(slot, at).start()

        if k == 0:
            swap_copy(last, spot).start()

    columns = [(2 * last, partner_column, None)]
    for slot, way, k in all_slots:
        columns.append((slot, chunk(way, k) * PAIR + side, (way, k)))
        columns.append((last + slot, chunk(way, k) * PAIR + 1 - side, (way, k)))

    def each(action):
        for slot, column, when in columns:
            if when is None:
                action(slot, column)
            else:

                @pl.when(arrives(*when))
                def _():
                    action(slot, column)

    def pass_on(slot, column):
        y_arrival(slot, column).wait_recv()
        e_copy(slot, column, across).start()

    def finish(slot, column):
        sib_mine = group * 2 + 1 - core
        sib_across = (1 - group) * 2 + 1 - core
        d_copy(slot, column, sib_mine).wait_recv()
        e_copy(slot, column, sib_across).wait_recv()
        y_copy(slot, column).wait_send()
        d_copy(slot, column, mine).wait_send()
        e_copy(slot, column, across).wait_send()

    each(pass_on)
    each(finish)
    for slot, way, k in all_slots:

        @pl.when(arrives(way, k))
        def _():
            at = chunk(way, k)
            swap_arrival(slot, at).wait_recv()
            swap_copy(slot, at).wait_send()
            column = at * PAIR + side
            pair_copy(slot, column, wf(column, mine)).wait_send()

        @pl.when(leaves(way, k))
        def _():
            at = carried(way, k)
            out_copy(way, k, at).wait_send()
            for p in range(PIECES):
                hid_copy(way, k, p, at).wait_send()

    swap_arrival(last, spot).wait_recv()
    swap_copy(last, spot).wait_send()
    pair_copy(last, rank, own_quarter).wait_send()
    w_out.wait_send()
    w_side.wait_send()
    keep.wait()
    for o in range(ranks - 1):
        send(
            fv_ref.at[:, pl.ds(0, head)], fo_ref.at[(rank + ranks - 1 - o) % ranks],
            fs_sem.at[o], fr_sem.at[o], peers[o],
        ).wait_recv()
    for copy in first_copies:
        copy.wait_send()


def exchange(ranks, att_ref, kept_ref, load_sem, s_sem, r_sem):
    group, core, rank = lax.axis_index("groups"), lax.axis_index("dp"), lax.axis_index("tensor")
    rows, head = kept_ref.shape[0], att_ref.shape[1]
    peers = [(group, core, (rank + o) % ranks) for o in range(1, ranks)]
    barrier = pltpu.get_barrier_semaphore()
    for there in peers:
        pl.semaphore_signal(barrier, inc=1, device_id=there, device_id_type=MESH)
    pl.semaphore_wait(barrier, ranks - 1)

    def block(r):
        return att_ref.at[pl.ds(pl.multiple_of(r * rows, rows), rows), :]

    def column(r):
        return kept_ref.at[:, pl.ds(pl.multiple_of(r * head, head), head)]

    def copy(o, r):
        return pltpu.make_async_remote_copy(
            src_ref=block(peers[o][2]), dst_ref=column(r), send_sem=s_sem.at[o], recv_sem=r_sem.at[o],
            device_id=peers[o], device_id_type=MESH,
        )

    for o in range(ranks - 1):
        copy(o, rank).start()
    own = pltpu.make_async_copy(block(rank), column(rank), load_sem)
    own.start()
    own.wait()
    for o in range(ranks - 1):
        copy(o, (rank + ranks - 1 - o) % ranks).wait_recv()
    for o in range(ranks - 1):
        copy(o, rank).wait_send()


def to_positions(attended, ranks):
    total_rows, head_width = attended.shape
    dma = pltpu.SemaphoreType.DMA
    return pl.pallas_call(
        functools.partial(exchange, ranks),
        out_shape=jax.ShapeDtypeStruct((total_rows // ranks, ranks * head_width), attended.dtype),
        in_specs=[pl.BlockSpec(memory_space=pltpu.VMEM)],
        out_specs=pl.BlockSpec(memory_space=pltpu.VMEM),
        scratch_shapes=[dma, dma((ranks - 1,)), dma((ranks - 1,))],
        compiler_params=pltpu.CompilerParams(
            collective_id=1, has_side_effects=True, vmem_limit_bytes=8 * 1024 * 1024
        ),
    )(attended)


def gathered(local_rows, w3, out_weight, firsts, ranks):
    line = ranks // PAIR
    steps = line - 1
    own_rows, width = local_rows.shape
    head_width = w3.shape[2]
    kind = local_rows.dtype
    dma = pltpu.SemaphoreType.DMA
    slots, wide = 2 * steps + 1, 4 * steps + 1
    anywhere = pl.BlockSpec(memory_space=pltpu.HBM)
    return pl.pallas_call(
        functools.partial(gather_project, line),
        out_shape=(
            jax.ShapeDtypeStruct((3, line, PAIR, own_rows, head_width), kind),
            jax.ShapeDtypeStruct((ranks,) + out_weight.shape, kind),
            jax.ShapeDtypeStruct((ranks, own_rows, head_width), kind),
        ),
        in_specs=[anywhere] * 4,
        out_specs=(
            pl.BlockSpec(memory_space=pltpu.VMEM),
            anywhere,
            pl.BlockSpec(memory_space=pltpu.VMEM),
        ),
        scratch_shapes=[
            pltpu.VMEM((line, own_rows, width), kind),
            pltpu.VMEM(w3.shape[:2] + (2 * head_width,), kind),
            pltpu.VMEM(out_weight.shape, kind),
            pltpu.VMEM((slots, 3, own_rows, head_width), kind),
            dma((5,)),
            dma((2, steps, PIECES)), dma((2, steps, PIECES)),
            dma((2,)), dma((2,)),
            dma((2, steps)), dma((2, steps)),
            dma((slots,)), dma((slots,)),
            dma((wide,)), dma((wide,)),
            dma((wide,)), dma((wide,)),
            dma((wide,)), dma((wide,)),
            dma((slots,)), dma((slots,)),
            dma((ranks - 1,)), dma((ranks - 1,)),
        ],
        compiler_params=pltpu.CompilerParams(
            collective_id=0, has_side_effects=True, vmem_limit_bytes=48 * 1024 * 1024
        ),
    )(local_rows, w3, out_weight, firsts)


def mix(values, firsts, mix_table, mix_index):
    levels = mix_table.shape[0]
    one_hot = (mix_index[:, None] == jnp.arange(levels, dtype=jnp.int32)[None, :]).astype(
        jnp.float32
    )
    weights_mix = jnp.dot(one_hot, mix_table, precision=lax.Precision.HIGHEST)
    return (
        weights_mix[None, :, 0:1] * values.astype(jnp.float32)
        + weights_mix[None, :, 1:2] * firsts.astype(jnp.float32)
    ).astype(jnp.bfloat16)


def body_gathered(hidden_in, first_values, qkv_weight, out_weight, mix_table, mix_index, lengths):
    local_rows = hidden_in[0]
    own_rows = local_rows.shape[0]
    ranks = lax.axis_size("tensor")
    total_rows = ranks * own_rows
    heads_here = mix_index.shape[0]
    head_width = qkv_weight.shape[2]
    head_size = head_width // heads_here
    qkv, full_out, relaid = gathered(
        local_rows, qkv_weight.transpose(1, 0, 2), out_weight, first_values[0], ranks
    )
    firsts = relaid.reshape(total_rows, heads_here, head_size)
    qkv = qkv.reshape(3, total_rows, heads_here, head_size)
    mixed_values = mix(qkv[2], firsts, mix_table, mix_index)
    attended = attention(qkv[0], qkv[1], mixed_values, lengths[0], head_size)
    attended = attended.reshape(total_rows, head_width)
    kept = to_positions(attended, ranks)
    weights = full_out.reshape(ranks * head_width, full_out.shape[2])
    return jnp.dot(kept, weights, preferred_element_type=jnp.float32).astype(jnp.bfloat16)[None]


def chosen(hidden_in, first_values, qkv_weight, out_weight, mix_table, mix_index, lengths):
    args = (hidden_in, first_values, qkv_weight, out_weight, mix_table, mix_index, lengths)
    ranks = lax.axis_size("tensor")
    total_rows = ranks * hidden_in.shape[1]
    fits = ranks * out_weight.size * 2 <= total_rows * hidden_in.shape[2] * 4
    two = lax.axis_size("groups") == 2 and lax.axis_size("dp") == 2
    if fits and two:
        return body_gathered(*args)
    return body(*args)


def solution(mesh):
    placed = (
        P(("groups", "dp"), "tensor", None),
        P(("groups", "dp"), "tensor", None),
        P(None, None, "tensor"),
        P("tensor", None),
        P(),
        P("tensor"),
        P(("groups", "dp")),
    )
    return jax.shard_map(
        chosen,
        mesh=mesh,
        in_specs=placed,
        out_specs=P(("groups", "dp"), "tensor", None),
        check_vma=False,
    )
```
